32 devices in a mesh: dp: 32 (over z, y, x, core).
Axes of the slice: x: 2, y: 2, z: 4, core: 2. Of those that a mesh axis runs over, the one named last changes fastest.
Arguments:
- tokens: bfloat16 [32768, 768], P('dp'), may hold values from -6 to 6
- lengths: int32 [32], P('dp'), may hold values from 256 to 1024, as said below
- drops: int32 [32], P('dp'), may hold values 0 or 1
- cotangent: bfloat16 [32768, 768], P('dp'), may hold values from -6 to 6
- w_qkv: bfloat16 [768, 2304], P('dp'), may hold values from -0.3125 to 0.3125
- w_out: bfloat16 [768, 768], P('dp'), may hold values from -1.75 to 1.75
- w_up: bfloat16 [768, 3072], P('dp'), may hold values from -0.21875 to 0.21875
- w_down: bfloat16 [3072, 768], P('dp'), may hold values from -0.109375 to 0.109375
- attn_vectors: bfloat16 [768, 5], P('dp'), may hold values from 0.25 to 1.75
- ffn_vectors: bfloat16 [768, 3], P('dp'), may hold values from 0.25 to 1.75
- up_bias: bfloat16 [3072], P('dp'), may hold values from -3 to 3
Outputs:
- result: bfloat16 [32768, 768], P('dp')
- grad_tokens: float32 [32768, 768], P('dp')
- grad_w_qkv: float32 [768, 2304], P('dp')
- grad_w_out: float32 [768, 768], P('dp')
- grad_w_up: float32 [768, 3072], P('dp')
- grad_w_down: float32 [3072, 768], P('dp')
- grad_attn_vectors: float32 [768, 5], P('dp')
- grad_ffn_vectors: float32 [768, 3], P('dp')
- grad_up_bias: float32 [3072], P('dp')
The draws below stay inside these ranges and needn't reach their ends.
Inputs may be any that keep to these rules, and one draw needn't show every extreme that they name: `lengths`: each sequence has 256 to 1024 real tokens; at least one sequence fills all its slots.
All inputs are finite; a program needn't handle non-finite values. No bound on the sum of `drops` on one device may be relied on, other than what follows from the above.
Results may differ from the reference program's by a relative error of at most 0.014.
The reference program's roundings to bfloat16 on the way count: a program that leaves them out, or rounds other values in their place, can miss the bound.
Values may be sent and summed in bfloat16 or wider, within the bound.
A program may use at most 256 MiB of HBM per device.

```python
import jax
import jax.numpy as jnp
from jax import lax

D = 768
H = 12
HD = 64
FF = 3072
SEQ = 1024
BLOCK = 512
SEQS = 32
TOKENS = 32768


def draw_lengths(key, part):
    base_lengths = jax.random.randint(key, (SEQS,), SEQ // 4, SEQ + 1)
    full_index = jax.random.randint(jax.random.fold_in(key, 7), (), 0, SEQS)
    return jnp.where(jnp.arange(SEQS) == full_index, SEQ, base_lengths).astype(jnp.int32)


def place_ends(entries, own_key, low, top_value):
    spot = [jax.random.randint(jax.random.fold_in(own_key, axis), (), 0, length) for axis, length in enumerate(entries.shape)]
    widest = entries.shape.index(max(entries.shape))
    beside = spot[:widest] + [(spot[widest] + 1) % entries.shape[widest]] + spot[widest + 1:]
    return entries.at[tuple(spot)].set(low).at[tuple(beside)].set(top_value)


def shard_levels(rng, shape, shards, smallest, top_value):
    gain = 1.0
    for position, blocks in shards:
        heights = jax.random.uniform(jax.random.fold_in(jax.random.fold_in(rng, 6), position), (blocks,), jnp.float32, smallest / len(shards), top_value / len(shards))
        gain = gain * jnp.repeat(jnp.exp(heights), shape[position] // blocks).reshape((-1,) + (1,) * (len(shape) - 1 - position))
    return gain


def scatter_about(rng, shape, scale, bound, pieces=(), kind=jnp.bfloat16):
    values = jax.random.normal(rng, shape, jnp.float32) * scale
    if len(pieces) > 0:
        values = shard_levels(rng, shape, pieces, -0.22, 0.18) * values
    return jnp.clip(values, min=-bound, max=bound).astype(kind)


def setup_inputs(seed: int = 0) -> dict:
    splits = jax.random.split(jax.random.key(seed), 12)
    return {
        "tokens": scatter_about(splits[0], (TOKENS, D), 1.0, 6.0, ((0, 32),)),
        "lengths": draw_lengths(jax.random.fold_in(splits[11], 71), 0),
        "drops": place_ends((jax.random.randint(splits[2], (SEQS,), 0, 4) < 1).astype(jnp.int32), jax.random.fold_in(splits[2], 1), 0, 1),
        "cotangent": scatter_about(splits[3], (TOKENS, D), 1.0, 6.0, ((0, 32),)),
        "w_qkv": scatter_about(splits[4], (D, 3 * D), (D // 2) ** -0.5, 0.3125, ((0, 32),)),
        "w_out": scatter_about(splits[5], (D, D), (D // 64) ** -0.5, 1.75, ((0, 32),)),
        "w_up": scatter_about(splits[6], (D, FF), D ** -0.5, 0.21875, ((0, 32),)),
        "w_down": scatter_about(splits[7], (FF, D), FF ** -0.5, 0.109375, ((0, 32),)),
        "attn_vectors": jnp.clip(1.0 + 0.15 * jax.random.normal(splits[8], (D, 5), jnp.float32), 0.25, 1.75).astype(jnp.bfloat16),
        "ffn_vectors": jnp.clip(1.0 + 0.15 * jax.random.normal(splits[9], (D, 3), jnp.float32), 0.25, 1.75).astype(jnp.bfloat16),
        "up_bias": scatter_about(splits[10], (FF,), 0.5, 3.0, ((0, 32),)),
    }


EPSILON = 1e-05
NEGATIVE = -1e+30

@jax.custom_vjp
def low(v):
    return lax.optimization_barrier(v.astype(jnp.bfloat16)).astype(jnp.float32)

@jax.custom_vjp
def low_back(v):
    return v

def low_keep(v):
    return (low(v), None)

def low_pass(kept, grad):
    return (grad,)

def back_keep(v):
    return (v, None)

def back_low(kept, grad):
    return (low(grad),)
low.defvjp(low_keep, low_pass)
low_back.defvjp(back_keep, back_low)

def normalize(hidden, gain_vec, shift_vec):
    row_mean = lax.optimization_barrier(jnp.mean(hidden, axis=-1, keepdims=True))
    centered = hidden - row_mean
    variance = lax.optimization_barrier(jnp.mean(centered * centered, axis=-1, keepdims=True))
    return centered * lax.rsqrt(variance + EPSILON) * gain_vec + shift_vec

def forward(inputs, w_qkv, w_out, w_up, w_down, attn_vectors, ffn_vectors, up_bias, length, drop_flag):
    highest = lax.Precision.HIGHEST
    positions = jnp.arange(SEQ, dtype=jnp.int32)
    key_live = positions < length
    valid = key_live.astype(inputs.dtype)[:, None]
    keep_flag = (1 - drop_flag).astype(inputs.dtype)
    inv_root = HD ** (-0.5)
    qkv_bias = jnp.concatenate([attn_vectors[:, 0], jnp.zeros((D,), inputs.dtype), attn_vectors[:, 1]])
    projected = low(low_back(jnp.dot(inputs, w_qkv, precision=highest) + qkv_bias))
    queries = projected[:, :D].reshape(SEQ // BLOCK, BLOCK, H, HD)
    keys_all = projected[:, D:2 * D].reshape(SEQ, H, HD)
    values_all = projected[:, 2 * D:].reshape(SEQ, H, HD)

    def attend(query_block):
        scores = low_back(jnp.einsum('bhd,khd->hbk', query_block, keys_all, precision=highest) * inv_root)
        scores = jnp.where(key_live[None, None, :], scores, NEGATIVE)
        probs = low(jax.nn.softmax(scores, axis=-1))
        return jnp.einsum('hbk,khd->bhd', probs, values_all, precision=highest)
    mixed = lax.map(jax.checkpoint(attend), queries).reshape(SEQ, D)
    heads_out = low(low_back(mixed))
    attn_res = low_back(jnp.dot(heads_out, w_out, precision=highest) + attn_vectors[:, 2])
    normed_one = normalize(inputs + attn_res, attn_vectors[:, 3], attn_vectors[:, 4])
    pre_act = low_back(jnp.dot(low(normed_one), w_up, precision=highest) + up_bias)
    activated = low(jax.nn.gelu(pre_act, approximate=False))
    ffn_res = low_back(jnp.dot(activated, w_down, precision=highest) + ffn_vectors[:, 0])
    layer_out = normalize(normed_one + ffn_res, ffn_vectors[:, 1], ffn_vectors[:, 2])
    return valid * (keep_flag * layer_out + (1 - keep_flag) * inputs)

def reference(tokens, lengths, drops, cotangent, w_qkv, w_out, w_up, w_down, attn_vectors, ffn_vectors, up_bias):
    weights = tuple((w.astype(jnp.float32) for w in (w_qkv, w_out, w_up, w_down, attn_vectors, ffn_vectors, up_bias)))
    seq_inputs = tokens.astype(jnp.float32).reshape(SEQS, SEQ, D)
    seq_grads = cotangent.astype(jnp.float32).reshape(SEQS, SEQ, D)

    def per_sequence(running, sequence_in):
        inputs, grads_in, length, drop_flag = sequence_in
        layer_fn = lambda x_in, *ws: forward(x_in, *ws, length, drop_flag)
        output, pullback = jax.vjp(layer_fn, inputs, *weights)
        grads = pullback(grads_in)
        running = tuple((r + g for r, g in zip(running, grads[1:])))
        return (running, (output.astype(jnp.bfloat16), grads[0]))
    init = tuple((jnp.zeros_like(w) for w in weights))
    totals, (outputs, grad_inputs) = lax.scan(per_sequence, init, (seq_inputs, seq_grads, lengths, drops))
    return (outputs.reshape(TOKENS, D), grad_inputs.reshape(TOKENS, D), totals[0], totals[1], totals[2], totals[3], totals[4], totals[5], totals[6])
```

```python
import functools

import jax
import jax.numpy as jnp
from jax import lax
from jax.experimental import pallas as pl
from jax.experimental.pallas import tpu as pltpu
from jax.sharding import PartitionSpec as P

MESH = pl.DeviceIdType.MESH
GRID = (4, 2, 2, 2)
LANES = 128
ANY = pl.BlockSpec(memory_space=pl.ANY)
VMEM = pl.BlockSpec(memory_space=pltpu.VMEM)


def place():
    me = lax.axis_index("dp")
    return me // 8, (me // 4) % 2, (me // 2) % 2, me % 2


def device(z, y, x, c):
    return ((z * 2 + y) * 2 + x) * 2 + c


def remote(src, dst, send, recv, to):
    return pltpu.make_async_remote_copy(
        src_ref=src, dst_ref=dst, send_sem=send, recv_sem=recv, device_id=(to,), device_id_type=MESH
    )


def meet(z, y, x, c):
    barrier = pltpu.get_barrier_semaphore()
    others = [device((z + k) % 4, y, x, c) for k in (1, 2, 3)]
    others += [device(z, 1 - y, x, c), device(z, y, 1 - x, c), device(z, y, x, 1 - c)]
    for other in others:
        pl.semaphore_signal(barrier, inc=1, device_id=(other,), device_id_type=MESH)
    pl.semaphore_wait(barrier, len(others))


def gather_kernel(count, *refs):
    shards, outs = refs[:count], refs[count : 2 * count]
    send, recv, local = refs[2 * count :]
    z, y, x, c = place()
    meet(z, y, x, c)
    y_to, x_to, c_to = device(z, 1 - y, x, c), device(z, y, 1 - x, c), device(z, y, x, 1 - c)
    low, high = pl.ds(0, 2), pl.ds(2, 2)
    every, both = pl.ds(0, 4), pl.ds(0, 2)
    arrays = range(count)

    def copy(w, slot, where, to):
        return remote(outs[w].at[where], outs[w].at[where], send.at[w, slot], recv.at[w, slot], to)

    pending = []

    def go(w, slot, where, to):
        one = copy(w, slot, where, to)
        one.start()
        pending.append(one)

    def arrived(w, slot, where):
        copy(w, slot, where, c_to).wait_recv()

    own = [pltpu.make_async_copy(shards[w], outs[w].at[z, y, x, c], local.at[w]) for w in arrays]
    for w in arrays:
        own[w].start()
        for k in (1, 2, 3):
            one = remote(
                shards[w],
                outs[w].at[z, y, x, c],
                send.at[w, k - 1],
                recv.at[w, k - 1],
                device((z + k) % 4, y, x, c),
            )
            one.start()
            pending.append(one)
    for w in arrays:
        own[w].wait()
        for k in (1, 2, 3):
            arrived(w, k - 1, ((z + 4 - k) % 4, y, x, c))
        go(w, 3, (low, y, x, c), x_to)
        go(w, 4, (high, y, x, c), y_to)
        go(w, 7, (every, y, x, c), c_to)
    for w in arrays:
        arrived(w, 3, (low, y, 1 - x, c))
        go(w, 5, (low, y, both, c), y_to)
        go(w, 8, (low, y, 1 - x, c), c_to)
        arrived(w, 4, (high, 1 - y, x, c))
        go(w, 6, (high, both, x, c), x_to)
        go(w, 9, (high, 1 - y, x, c), c_to)
    for w in arrays:
        arrived(w, 5, (low, 1 - y, both, c))
        go(w, 10, (low, 1 - y, both, c), c_to)
        arrived(w, 6, (high, both, 1 - x, c))
        go(w, 11, (high, both, 1 - x, c), c_to)
    for w in arrays:
        arrived(w, 7, (every, y, x, 1 - c))
        arrived(w, 8, (low, y, 1 - x, 1 - c))
        arrived(w, 9, (high, 1 - y, x, 1 - c))
        arrived(w, 10, (low, 1 - y, both, 1 - c))
        arrived(w, 11, (high, both, 1 - x, 1 - c))
    for one in pending:
        one.wait_send()


def gather(shards):
    count = len(shards)
    return pl.pallas_call(
        functools.partial(gather_kernel, count),
        out_shape=[jax.ShapeDtypeStruct(GRID + s.shape, s.dtype) for s in shards],
        in_specs=[VMEM] * count,
        out_specs=[ANY] * count,
        scratch_shapes=[
            pltpu.SemaphoreType.DMA((count, 12)),
            pltpu.SemaphoreType.DMA((count, 12)),
            pltpu.SemaphoreType.DMA((count,)),
        ],
        compiler_params=pltpu.CompilerParams(
            collective_id=0, has_side_effects=True, vmem_limit_bytes=8 << 20
        ),
        name="gather_weights",
    )(*shards)


def scatter_kernel(count, *refs):
    grads, sums = refs[:count], refs[count : 2 * count]
    groups = [refs[2 * count + 7 * w : 2 * count + 7 * (w + 1)] for w in range(count)]
    send, recv, local = refs[9 * count :]
    z, y, x, c = place()
    meet(z, y, x, c)
    y_to, x_to, c_to = device(z, 1 - y, x, c), device(z, y, 1 - x, c), device(z, y, x, 1 - c)
    low, high = pl.ds(0, 2), pl.ds(2, 2)
    every, both = pl.ds(0, 4), pl.ds(0, 2)
    arrays = range(count)
    f32 = jnp.float32
    pending = []

    def go(src, dst, w, slot, to):
        one = remote(src, dst, send.at[w, slot], recv.at[w, slot], to)
        one.start()
        pending.append(one)
        return one

    def add(dst, src, total):
        def step(i, carry):
            a, b = dst(i), src(i)
            a[...] = (a[...].astype(f32) + b[...].astype(f32)).astype(a.dtype)
            return carry

        lax.fori_loop(0, total, step, 0)

    own, first = [], []
    for w in arrays:
        acc, r0 = groups[w][:2]
        first.append(go(grads[w].at[every, both, both, 1 - c], r0, w, 0, c_to))
        one = pltpu.make_async_copy(grads[w].at[every, both, both, c], acc, local.at[w])
        one.start()
        own.append(one)
    second = []
    for w in arrays:
        acc, r0, r1a, r1b, r2a, r2b, r3 = groups[w]
        own[w].wait()
        first[w].wait_recv()
        add(
            lambda i: acc.at[i // 4, (i // 2) % 2, i % 2],
            lambda i: r0.at[i // 4, (i // 2) % 2, i % 2],
            16,
        )
        second.append(
            (
                go(acc.at[low, both, 1 - x], r1a, w, 1, x_to),
                go(acc.at[high, 1 - y, both], r1b, w, 2, y_to),
            )
        )
    third = []
    for w in arrays:
        acc, r0, r1a, r1b, r2a, r2b, r3 = groups[w]
        second[w][0].wait_recv()
        add(lambda i: acc.at[i // 2, i % 2, x], lambda i: r1a.at[i // 2, i % 2], 4)
        a = go(acc.at[low, 1 - y, x], r2a, w, 3, y_to)
        second[w][1].wait_recv()
        add(lambda i: acc.at[2 + i // 2, y, i % 2], lambda i: r1b.at[i // 2, i % 2], 4)
        b = go(acc.at[high, y, 1 - x], r2b, w, 4, x_to)
        third.append((a, b))
    last = []
    for w in arrays:
        acc, r0, r1a, r1b, r2a, r2b, r3 = groups[w]
        third[w][0].wait_recv()
        add(lambda i: acc.at[i, y, x], lambda i: r2a.at[i], 2)
        third[w][1].wait_recv()
        add(lambda i: acc.at[2 + i, y, x], lambda i: r2b.at[i], 2)
        last.append(
            [
                go(
                    acc.at[(z + k) % 4, y, x],
                    r3.at[k - 1],
                    w,
                    4 + k,
                    device((z + k) % 4, y, x, c),
                )
                for k in (1, 2, 3)
            ]
        )
    for w in arrays:
        acc, r0, r1a, r1b, r2a, r2b, r3 = groups[w]
        for one in last[w]:
            one.wait_recv()
        sums[w][...] = (
            (acc[z, y, x].astype(f32) + r3[0].astype(f32))
            + (r3[1].astype(f32) + r3[2].astype(f32))
        )
    for one in pending:
        one.wait_send()


def scatter(grads):
    count = len(grads)
    scratch = []
    for g in grads:
        rows = g.shape[4]
        bf16 = g.dtype
        for shape in ((4, 2, 2), (4, 2, 2), (2, 2), (2, 2), (2,), (2,), (3,)):
            scratch.append(pltpu.VMEM(shape + (rows, LANES), bf16))
    return pl.pallas_call(
        functools.partial(scatter_kernel, count),
        out_shape=[jax.ShapeDtypeStruct(g.shape[4:], jnp.float32) for g in grads],
        in_specs=[ANY] * count,
        out_specs=[VMEM] * count,
        scratch_shapes=scratch
        + [
            pltpu.SemaphoreType.DMA((count, 8)),
            pltpu.SemaphoreType.DMA((count, 8)),
            pltpu.SemaphoreType.DMA((count,)),
        ],
        compiler_params=pltpu.CompilerParams(
            collective_id=1, has_side_effects=True, vmem_limit_bytes=40 << 20
        ),
        name="scatter_grads",
    )(*grads)


def as_slabs(grad):
    rows, cols = grad.shape[0] // 32, grad.shape[1]
    tiles = grad.reshape(32, rows // 8, 8, cols // LANES, LANES).transpose(0, 1, 3, 2, 4)
    return tiles.reshape(GRID + (rows * cols // LANES, LANES))


def from_slab(slab, rows, cols):
    tiles = slab.reshape(rows // 8, cols // LANES, 8, LANES).transpose(0, 2, 1, 3)
    return tiles.reshape(rows, cols)


H = 12
BLOCK = 512


EPSILON = 1e-05
NEGATIVE = -1e30


def normalize(hidden, gain_vec, shift_vec):
    row_mean = jnp.mean(hidden, axis=-1, keepdims=True)
    centered = hidden - row_mean
    variance = jnp.mean(centered * centered, axis=-1, keepdims=True)
    return centered * lax.rsqrt(variance + EPSILON) * gain_vec + shift_vec


def gelu_exact(inputs):
    return jax.nn.gelu(inputs, approximate=False)


def fetch_plain(*shards):
    return tuple(lax.all_gather(s, "dp", axis=0, tiled=True) for s in shards)


def spread_plain(*grads):
    return tuple(lax.psum_scatter(g, "dp", scatter_dimension=0, tiled=True) for g in grads)


def fetch_kernel(w_qkv, w_out, w_up, w_down, attn_vectors, ffn_vectors, up_bias):
    small = jnp.concatenate([attn_vectors.reshape(-1), ffn_vectors.reshape(-1), up_bias])
    small = jnp.pad(small, (0, 16 * LANES - small.shape[0])).reshape(16, LANES)
    full = gather([w_qkv, w_out, w_up, w_down, small])
    weights = [f.reshape(-1, f.shape[-1]) for f in full[:4]]
    small = full[4].reshape(32, 16 * LANES)
    return (
        *weights,
        small[:, :120].reshape(-1, 5),
        small[:, 120:192].reshape(-1, 3),
        small[:, 192:288].reshape(-1),
    )


def spread_kernel(g_qkv, g_out, g_up, g_down, g_avec, g_fvec, g_bias):
    small = jnp.concatenate(
        [g_avec.reshape(32, 120), g_fvec.reshape(32, 72), g_bias.reshape(32, 96)], axis=1
    )
    small = jnp.pad(small, ((0, 0), (0, 16 * LANES - 288))).astype(jnp.bfloat16)
    big = [as_slabs(g.astype(jnp.bfloat16)) for g in (g_qkv, g_out, g_up, g_down)]
    s_qkv, s_out, s_up, s_down, s_small = scatter(big + [small.reshape(GRID + (16, LANES))])
    flat = s_small.reshape(-1)
    return (
        from_slab(s_qkv, 24, 2304),
        from_slab(s_out, 24, 768),
        from_slab(s_up, 24, 3072),
        from_slab(s_down, 96, 768),
        flat[:120].reshape(24, 5),
        flat[120:192].reshape(24, 3),
        flat[192:288],
    )


def local(
    fetch,
    spread,
    tokens,
    lengths,
    drops,
    cotangent,
    w_qkv,
    w_out,
    w_up,
    w_down,
    attn_vectors,
    ffn_vectors,
    up_bias,
):
    f32 = jnp.float32
    bf16 = jnp.bfloat16
    seq_len, width = tokens.shape
    head_dim = width // H
    inv_root = head_dim ** (-0.5)
    n_blocks = seq_len // BLOCK
    positions = jnp.arange(seq_len, dtype=jnp.int32)
    key_live = positions < lengths[0]
    valid = key_live.astype(f32)[:, None]
    keep_flag = (1 - drops[0]).astype(f32)
    (qkv_full, out_full, up_full, down_full, avec_low, fvec_low, bias_low) = fetch(
        w_qkv, w_out, w_up, w_down, attn_vectors, ffn_vectors, up_bias
    )
    avec = avec_low.astype(f32)
    fvec = fvec_low.astype(f32)
    bias_up = bias_low.astype(f32)
    inputs = tokens.astype(f32)
    qkv_bias = jnp.concatenate([avec[:, 0], jnp.zeros((width,), f32), avec[:, 1]])
    projected = (jnp.dot(tokens, qkv_full, preferred_element_type=f32) + qkv_bias).astype(bf16)
    queries = projected[:, :width].reshape(n_blocks, BLOCK, H, head_dim)
    keys_all = projected[:, width : 2 * width].reshape(seq_len, H, head_dim)
    values_all = projected[:, 2 * width :].reshape(seq_len, H, head_dim)

    def scores_of(query_block):
        raw_scores = (
            jnp.einsum("bhd,khd->hbk", query_block, keys_all, preferred_element_type=f32) * inv_root
        )
        return jnp.where(key_live[None, None, :], raw_scores, NEGATIVE)

    def attend(query_block):
        scores = scores_of(query_block)
        top_score = jnp.max(scores, axis=-1, keepdims=True)
        expo = jnp.exp(scores - top_score)
        totals = jnp.sum(expo, axis=-1, keepdims=True)
        probs = (expo / totals).astype(bf16)
        mixed = jnp.einsum("hbk,khd->bhd", probs, values_all, preferred_element_type=f32)
        return (mixed, top_score[..., 0] + jnp.log(totals[..., 0]))

    mixed, log_sums = lax.map(attend, queries)
    heads_out = mixed.reshape(seq_len, width).astype(bf16)
    attn_res = jnp.dot(heads_out, out_full, preferred_element_type=f32) + avec[:, 2]
    first_sum = inputs + attn_res
    normed_one, norm_one_back = jax.vjp(normalize, first_sum, avec[:, 3], avec[:, 4])
    normed_low = normed_one.astype(bf16)
    pre_act = jnp.dot(normed_low, up_full, preferred_element_type=f32) + bias_up
    activated, gelu_back = jax.vjp(gelu_exact, pre_act)
    act_low = activated.astype(bf16)
    ffn_res = jnp.dot(act_low, down_full, preferred_element_type=f32) + fvec[:, 0]
    second_sum = normed_one + ffn_res
    layer_out, norm_two_back = jax.vjp(normalize, second_sum, fvec[:, 1], fvec[:, 2])
    result = (valid * (keep_flag * layer_out + (1 - keep_flag) * inputs)).astype(bf16)
    grad_output = valid * cotangent.astype(f32)
    grad_layer = keep_flag * grad_output
    grad_second, grad_gain_two, grad_shift_two = norm_two_back(grad_layer)
    grad_ffn = grad_second.astype(bf16)
    grad_down = jnp.einsum("tf,td->fd", act_low, grad_ffn, preferred_element_type=f32)
    grad_bias_two = jnp.sum(grad_ffn, axis=0, dtype=f32)
    ffn_vec_grad = jnp.stack([grad_bias_two, grad_gain_two, grad_shift_two], axis=1)
    grad_act = jnp.einsum("td,fd->tf", grad_ffn, down_full, preferred_element_type=f32)
    grad_pre = gelu_back(grad_act)[0].astype(bf16)
    grad_up = jnp.einsum("td,tf->df", normed_low, grad_pre, preferred_element_type=f32)
    grad_bias_up = jnp.sum(grad_pre, axis=0, dtype=f32)
    grad_normed = grad_second + jnp.einsum(
        "tf,df->td", grad_pre, up_full, preferred_element_type=f32
    )
    grad_first, grad_gain_one, grad_shift_one = norm_one_back(grad_normed)
    grad_attn = grad_first.astype(bf16)
    grad_bias_out = jnp.sum(grad_attn, axis=0, dtype=f32)
    grad_wout = jnp.einsum("td,te->de", heads_out, grad_attn, preferred_element_type=f32)
    grad_heads = jnp.einsum("te,de->td", grad_attn, out_full, preferred_element_type=f32).astype(
        bf16
    )
    grad_heads = grad_heads.reshape(n_blocks, BLOCK, H, head_dim)

    def back_block(running, block_in):
        grad_keys, grad_values = running
        query_block, grad_block, lse_block = block_in
        scores = scores_of(query_block)
        probs = jnp.exp(scores - lse_block[..., None])
        grad_probs = jnp.einsum("bhd,khd->hbk", grad_block, values_all, preferred_element_type=f32)
        row_delta = jnp.sum(probs * grad_probs, axis=-1, keepdims=True)
        grad_scores = (probs * (grad_probs - row_delta)).astype(bf16)
        grad_query = (
            jnp.einsum("hbk,khd->bhd", grad_scores, keys_all, preferred_element_type=f32) * inv_root
        )
        grad_keys = (
            grad_keys
            + jnp.einsum("hbk,bhd->khd", grad_scores, query_block, preferred_element_type=f32)
            * inv_root
        )
        grad_values = grad_values + jnp.einsum(
            "hbk,bhd->khd", probs.astype(bf16), grad_block, preferred_element_type=f32
        )
        return ((grad_keys, grad_values), grad_query)

    zero_heads = jnp.zeros((seq_len, H, head_dim), f32)
    (grad_keys, grad_values), grad_queries = lax.scan(
        back_block, (zero_heads, zero_heads), (queries, grad_heads, log_sums)
    )
    grad_proj = jnp.concatenate(
        [
            grad_queries.reshape(seq_len, width),
            grad_keys.reshape(seq_len, width),
            grad_values.reshape(seq_len, width),
        ],
        axis=1,
    ).astype(bf16)
    grad_qkv = jnp.einsum("td,te->de", tokens, grad_proj, preferred_element_type=f32)
    proj_sums = jnp.sum(grad_proj, axis=0, dtype=f32)
    attn_vec_grad = jnp.stack(
        [proj_sums[:width], proj_sums[2 * width :], grad_bias_out, grad_gain_one, grad_shift_one],
        axis=1,
    )
    sum_qkv, sum_wout, sum_up, sum_down, sum_avec, sum_fvec, sum_bias_up = spread(
        grad_qkv, grad_wout, grad_up, grad_down, attn_vec_grad, ffn_vec_grad, grad_bias_up
    )
    grad_inputs = grad_first + jnp.einsum(
        "te,de->td", grad_proj, qkv_full, preferred_element_type=f32
    )
    grad_tokens = keep_flag * grad_inputs + (1 - keep_flag) * grad_output
    return (
        result,
        grad_tokens,
        sum_qkv,
        sum_wout,
        sum_up,
        sum_down,
        sum_avec,
        sum_fvec,
        sum_bias_up,
    )


def solution(mesh):
    kernels = mesh.shape["dp"] == 32
    layer = functools.partial(
        local, fetch_kernel if kernels else fetch_plain, spread_kernel if kernels else spread_plain
    )
    return jax.shard_map(
        layer,
        mesh=mesh,
        in_specs=(
            P("dp", None),
            P("dp"),
            P("dp"),
            P("dp", None),
            P("dp", None),
            P("dp", None),
            P("dp", None),
            P("dp", None),
            P("dp", None),
            P("dp", None),
            P("dp"),
        ),
        out_specs=(
            P("dp", None),
            P("dp", None),
            P("dp", None),
            P("dp", None),
            P("dp", None),
            P("dp", None),
            P("dp", None),
            P("dp", None),
            P("dp"),
        ),
        check_vma=False,
    )
```

```python
import functools

import jax
import jax.numpy as jnp
from jax import lax
from jax.experimental import pallas as pl
from jax.experimental.pallas import tpu as pltpu
from jax.sharding import PartitionSpec as P

MESH = pl.DeviceIdType.MESH
GRID = (4, 2, 2, 2)
LANES = 128
ANY = pl.BlockSpec(memory_space=pl.ANY)
VMEM = pl.BlockSpec(memory_space=pltpu.VMEM)


def place():
    me = lax.axis_index("dp")
    return me // 8, (me // 4) % 2, (me // 2) % 2, me % 2


def device(z, y, x, c):
    return ((z * 2 + y) * 2 + x) * 2 + c


def remote(src, dst, send, recv, to):
    return pltpu.make_async_remote_copy(
        src_ref=src, dst_ref=dst, send_sem=send, recv_sem=recv, device_id=(to,), device_id_type=MESH
    )


def meet(z, y, x, c):
    barrier = pltpu.get_barrier_semaphore()
    others = [device((z + k) % 4, y, x, c) for k in (1, 2, 3)]
    others += [device(z, 1 - y, x, c), device(z, y, 1 - x, c), device(z, y, x, 1 - c)]
    for other in others:
        pl.semaphore_signal(barrier, inc=1, device_id=(other,), device_id_type=MESH)
    pl.semaphore_wait(barrier, len(others))


def gather_kernel(count, *refs):
    shards, outs = refs[:count], refs[count : 2 * count]
    send, recv, local = refs[2 * count :]
    z, y, x, c = place()
    meet(z, y, x, c)
    y_to, x_to, c_to = device(z, 1 - y, x, c), device(z, y, 1 - x, c), device(z, y, x, 1 - c)
    low, high = pl.ds(0, 2), pl.ds(2, 2)
    every, both = pl.ds(0, 4), pl.ds(0, 2)
    arrays = range(count)

    def copy(w, slot, where, to):
        return remote(outs[w].at[where], outs[w].at[where], send.at[w, slot], recv.at[w, slot], to)

    pending = []

    def go(w, slot, where, to):
        one = copy(w, slot, where, to)
        one.start()
        pending.append(one)

    def arrived(w, slot, where):
        copy(w, slot, where, c_to).wait_recv()

    own = [pltpu.make_async_copy(shards[w], outs[w].at[z, y, x, c], local.at[w]) for w in arrays]
    for w in arrays:
        own[w].start()
        for k in (1, 2, 3):
            one = remote(
                shards[w],
                outs[w].at[z, y, x, c],
                send.at[w, k - 1],
                recv.at[w, k - 1],
                device((z + k) % 4, y, x, c),
            )
            one.start()
            pending.append(one)
    for w in arrays:
        own[w].wait()
        for k in (1, 2, 3):
            arrived(w, k - 1, ((z + 4 - k) % 4, y, x, c))
        go(w, 3, (low, y, x, c), x_to)
        go(w, 4, (high, y, x, c), y_to)
        go(w, 7, (every, y, x, c), c_to)
    for w in arrays:
        arrived(w, 3, (low, y, 1 - x, c))
        go(w, 5, (low, y, both, c), y_to)
        go(w, 8, (low, y, 1 - x, c), c_to)
        arrived(w, 4, (high, 1 - y, x, c))
        go(w, 6, (high, both, x, c), x_to)
        go(w, 9, (high, 1 - y, x, c), c_to)
    for w in arrays:
        arrived(w, 5, (low, 1 - y, both, c))
        go(w, 10, (low, 1 - y, both, c), c_to)
        arrived(w, 6, (high, both, 1 - x, c))
        go(w, 11, (high, both, 1 - x, c), c_to)
    for w in arrays:
        arrived(w, 7, (every, y, x, 1 - c))
        arrived(w, 8, (low, y, 1 - x, 1 - c))
        arrived(w, 9, (high, 1 - y, x, 1 - c))
        arrived(w, 10, (low, 1 - y, both, 1 - c))
        arrived(w, 11, (high, both, 1 - x, 1 - c))
    for one in pending:
        one.wait_send()


def gather(shards):
    count = len(shards)
    return pl.pallas_call(
        functools.partial(gather_kernel, count),
        out_shape=[jax.ShapeDtypeStruct(GRID + s.shape, s.dtype) for s in shards],
        in_specs=[VMEM] * count,
        out_specs=[ANY] * count,
        scratch_shapes=[
            pltpu.SemaphoreType.DMA((count, 12)),
            pltpu.SemaphoreType.DMA((count, 12)),
            pltpu.SemaphoreType.DMA((count,)),
        ],
        compiler_params=pltpu.CompilerParams(
            collective_id=0, has_side_effects=True, vmem_limit_bytes=8 << 20
        ),
        name="gather_weights",
    )(*shards)


def scatter_kernel(count, *refs):
    grads, sums = refs[:count], refs[count : 2 * count]
    groups = [refs[2 * count + 7 * w : 2 * count + 7 * (w + 1)] for w in range(count)]
    send, recv, local = refs[9 * count :]
    z, y, x, c = place()
    meet(z, y, x, c)
    y_to, x_to, c_to = device(z, 1 - y, x, c), device(z, y, 1 - x, c), device(z, y, x, 1 - c)
    low, high = pl.ds(0, 2), pl.ds(2, 2)
    every, both = pl.ds(0, 4), pl.ds(0, 2)
    arrays = range(count)
    f32 = jnp.float32
    pending = []

    def go(src, dst, w, slot, to):
        one = remote(src, dst, send.at[w, slot], recv.at[w, slot], to)
        one.start()
        pending.append(one)
        return one

    def add(dst, src, total):
        def step(i, carry):
            a, b = dst(i), src(i)
            a[...] = (a[...].astype(f32) + b[...].astype(f32)).astype(a.dtype)
            return carry

        lax.fori_loop(0, total, step, 0)

    own, first = [], []
    for w in arrays:
        acc, r0 = groups[w][:2]
        first.append(go(grads[w].at[every, both, both, 1 - c], r0, w, 0, c_to))
        one = pltpu.make_async_copy(grads[w].at[every, both, both, c], acc, local.at[w])
        one.start()
        own.append(one)
    second = []
    for w in arrays:
        acc, r0, r1a, r1b, r2a, r2b, r3 = groups[w]
        own[w].wait()
        first[w].wait_recv()
        add(
            lambda i: acc.at[i // 4, (i // 2) % 2, i % 2],
            lambda i: r0.at[i // 4, (i // 2) % 2, i % 2],
            16,
        )
        second.append(
            (
                go(acc.at[low, both, 1 - x], r1a, w, 1, x_to),
                go(acc.at[high, 1 - y, both], r1b, w, 2, y_to),
            )
        )
    third = []
    for w in arrays:
        acc, r0, r1a, r1b, r2a, r2b, r3 = groups[w]
        second[w][0].wait_recv()
        add(lambda i: acc.at[i // 2, i % 2, x], lambda i: r1a.at[i // 2, i % 2], 4)
        a = go(acc.at[low, 1 - y, x], r2a, w, 3, y_to)
        second[w][1].wait_recv()
        add(lambda i: acc.at[2 + i // 2, y, i % 2], lambda i: r1b.at[i // 2, i % 2], 4)
        b = go(acc.at[high, y, 1 - x], r2b, w, 4, x_to)
        third.append((a, b))
    last = []
    for w in arrays:
        acc, r0, r1a, r1b, r2a, r2b, r3 = groups[w]
        third[w][0].wait_recv()
        add(lambda i: acc.at[i, y, x], lambda i: r2a.at[i], 2)
        third[w][1].wait_recv()
        add(lambda i: acc.at[2 + i, y, x], lambda i: r2b.at[i], 2)
        last.append(
            [
                go(
                    acc.at[(z + k) % 4, y, x],
                    r3.at[k - 1],
                    w,
                    4 + k,
                    device((z + k) % 4, y, x, c),
                )
                for k in (1, 2, 3)
            ]
        )
    for w in arrays:
        acc, r0, r1a, r1b, r2a, r2b, r3 = groups[w]
        for one in last[w]:
            one.wait_recv()
        sums[w][...] = (
            (acc[z, y, x].astype(f32) + r3[0].astype(f32))
            + (r3[1].astype(f32) + r3[2].astype(f32))
        )
    for one in pending:
        one.wait_send()


def scatter(grads):
    count = len(grads)
    scratch = []
    for g in grads:
        rows = g.shape[4]
        bf16 = g.dtype
        for shape in ((4, 2, 2), (4, 2, 2), (2, 2), (2, 2), (2,), (2,), (3,)):
            scratch.append(pltpu.VMEM(shape + (rows, LANES), bf16))
    return pl.pallas_call(
        functools.partial(scatter_kernel, count),
        out_shape=[jax.ShapeDtypeStruct(g.shape[4:], jnp.float32) for g in grads],
        in_specs=[ANY] * count,
        out_specs=[VMEM] * count,
        scratch_shapes=scratch
        + [
            pltpu.SemaphoreType.DMA((count, 8)),
            pltpu.SemaphoreType.DMA((count, 8)),
            pltpu.SemaphoreType.DMA((count,)),
        ],
        compiler_params=pltpu.CompilerParams(
            collective_id=1, has_side_effects=True, vmem_limit_bytes=40 << 20
        ),
        name="scatter_grads",
    )(*grads)


def as_slabs(grad):
    rows, cols = grad.shape[0] // 32, grad.shape[1]
    tiles = grad.reshape(32, rows // 8, 8, cols // LANES, LANES).transpose(0, 1, 3, 2, 4)
    return tiles.reshape(GRID + (rows * cols // LANES, LANES))


def from_slab(slab, rows, cols):
    tiles = slab.reshape(rows // 8, cols // LANES, 8, LANES).transpose(0, 2, 1, 3)
    return tiles.reshape(rows, cols)

H = 12
EPSILON = 1e-05

LOG2E = 1.4426950408889634
DEAD = -1e30


def exact_parts(value):
    low = jnp.bfloat16
    f32 = jnp.float32
    one = value.astype(low)
    rest = value - one.astype(f32)
    two = rest.astype(low)
    three = (rest - two.astype(f32)).astype(low)
    return one, two, three


def attend_kernel(head_dim, block, length_ref, q_ref, k_ref, v_ref, o_ref, lse_ref, qq, kk, vv):
    f32, bf16 = jnp.float32, jnp.bfloat16
    seq, width = q_ref.shape
    lane = lax.broadcasted_iota(jnp.int32, (1, width), 1)
    row = lax.broadcasted_iota(jnp.int32, (seq, 1), 0)
    first = lane < head_dim
    q = q_ref[...].astype(f32) * (head_dim**-0.5 * LOG2E)
    q_high = q.astype(bf16).astype(f32)
    q_low = q - q_high
    k, v = k_ref[...].astype(f32), v_ref[...].astype(f32)
    dead = jnp.where(row < length_ref[0], 0.0, DEAD)
    for h in (0, 1):
        data = first if h == 0 else lane >= head_dim
        spot = head_dim * (1 - h)
        qq[h, :, :width] = jnp.where(data, q_high, jnp.where(lane == spot, 1.0, 0.0)).astype(bf16)
        qq[h, :, width:] = jnp.where(data, q_low, 0.0).astype(bf16)
        kk[h, :, :width] = jnp.where(data, k, jnp.where(lane == spot, dead, 0.0)).astype(bf16)
        kk[h, :, width:] = k_ref[...]
        vv[h] = jnp.where(data, v, 1.0).astype(bf16)

    def one_block(i, carry):
        at = pl.ds(pl.multiple_of(i * block, block), block)
        outs, tops = [], []
        for h in (0, 1):
            s = lax.dot_general(
                qq[h, at], kk[h], (((1,), (1,)), ((), ())), preferred_element_type=f32
            )
            top = jnp.max(s, axis=1, keepdims=True)
            p = jnp.exp2(s - top).astype(bf16)
            outs.append(jnp.dot(p, vv[h], preferred_element_type=f32))
            tops.append(top)
        mixed = jnp.where(first, outs[0], outs[1])
        sums = jnp.where(first, outs[1], outs[0])
        o_ref[at, :] = (mixed / pltpu.roll(sums, head_dim, 1)).astype(bf16)
        lse_ref[at, :] = jnp.where(first, tops[1], tops[0]) + jnp.log2(sums)
        return carry

    lax.fori_loop(0, seq // block, one_block, 0)


def attend(length, proj, heads, block=512):
    seq, width = proj.shape[0], proj.shape[1] // 3
    pairs, head_dim = heads // 2, width // heads
    two = 2 * head_dim

    def part(n):
        return pl.BlockSpec((seq, two), lambda p: (0, n * pairs + p))

    out = pl.BlockSpec((seq, two), lambda p: (0, p))
    return pl.pallas_call(
        functools.partial(attend_kernel, head_dim, block),
        grid=(pairs,),
        out_shape=[
            jax.ShapeDtypeStruct((seq, width), jnp.bfloat16),
            jax.ShapeDtypeStruct((seq, width), jnp.float32),
        ],
        in_specs=[pl.BlockSpec(memory_space=pltpu.SMEM), part(0), part(1), part(2)],
        out_specs=[out, out],
        scratch_shapes=[
            pltpu.VMEM((2, seq, 2 * two), jnp.bfloat16),
            pltpu.VMEM((2, seq, 2 * two), jnp.bfloat16),
            pltpu.VMEM((2, seq, two), jnp.bfloat16),
        ],
        compiler_params=pltpu.CompilerParams(vmem_limit_bytes=48 << 20),
        name="attend_fwd",
    )(length, proj, proj, proj)


def attend_back_kernel(
    head_dim, block, length_ref, q_ref, k_ref, v_ref, do_ref, o_ref, lse_ref,
    dq_ref, dk_ref, dv_ref, qq, kk, vv, dd, dk_acc, dv_acc, kt,
):
    f32, bf16 = jnp.float32, jnp.bfloat16
    seq, width = q_ref.shape
    scale = head_dim**-0.5
    lane = lax.broadcasted_iota(jnp.int32, (1, width), 1)
    row = lax.broadcasted_iota(jnp.int32, (seq, 1), 0)
    first = lane < head_dim
    q = q_ref[...].astype(f32) * (scale * LOG2E)
    q_high = q.astype(bf16).astype(f32)
    q_low = q - q_high
    k, v, do = k_ref[...].astype(f32), v_ref[...].astype(f32), do_ref[...].astype(f32)
    dead = jnp.where(row < length_ref[0], 0.0, DEAD)
    swap_r = lax.broadcasted_iota(jnp.int32, (width, width), 0) < head_dim
    swap_c = lax.broadcasted_iota(jnp.int32, (width, width), 1) < head_dim
    swap = jnp.where(swap_r != swap_c, 1.0, 0.0).astype(bf16)
    terms = exact_parts(do * o_ref[...].astype(f32))
    delta = sum(jnp.dot(t, swap, preferred_element_type=f32) for t in terms)
    l_parts = [t.astype(f32) for t in exact_parts(-lse_ref[...])]
    d_parts = [t.astype(f32) for t in exact_parts(-delta)]
    kt[...] = k.T.astype(bf16)
    for h in (0, 1):
        data = first if h == 0 else lane >= head_dim
        spot = head_dim * (1 - h)

        def place(spots):
            value = 0.0
            for n, part in spots:
                value = jnp.where(lane == spot + n, part, value)
            return value

        qx = place([(0, 1.0)] + [(1 + n, l_parts[n]) for n in range(3)])
        kx = place([(0, dead)] + [(1 + n, 1.0) for n in range(3)])
        dx = place([(n, d_parts[n]) for n in range(3)])
        vx = place([(n, 1.0) for n in range(3)])
        qq[h, :, :width] = jnp.where(data, q_high, qx).astype(bf16)
        qq[h, :, width:] = jnp.where(data, q_low, 0.0).astype(bf16)
        kk[h, :, :width] = jnp.where(data, k, kx).astype(bf16)
        kk[h, :, width:] = k_ref[...]
        vv[h] = jnp.where(data, v, vx).astype(bf16)
        dd[h] = jnp.where(data, do, dx).astype(bf16)
    dk_acc[...] = jnp.zeros_like(dk_acc)
    dv_acc[...] = jnp.zeros_like(dv_acc)
    across = (((1,), (1,)), ((), ()))

    def one_block(i, carry):
        at = pl.ds(pl.multiple_of(i * block, block), block)
        turned = []
        for h in (0, 1):
            p = jnp.exp2(lax.dot_general(kk[h], qq[h, at], across, preferred_element_type=f32))
            dp = lax.dot_general(vv[h], dd[h, at], across, preferred_element_type=f32)
            ds = (p * dp).astype(bf16)
            dv_acc[h] += jnp.dot(p.astype(bf16), do_ref[at, :], preferred_element_type=f32)
            dk_acc[h] += jnp.dot(ds, q_ref[at, :], preferred_element_type=f32)
            turned.append(
                jnp.dot(
                    kt[pl.ds(h * head_dim, head_dim), :], ds, preferred_element_type=f32
                )
            )
        dq = jnp.concatenate(turned, axis=0).T
        dq_ref[at, :] = (dq * scale).astype(bf16)
        return carry

    lax.fori_loop(0, seq // block, one_block, 0)
    dk_ref[...] = (jnp.where(first, dk_acc[0], dk_acc[1]) * scale).astype(bf16)
    dv_ref[...] = jnp.where(first, dv_acc[0], dv_acc[1]).astype(bf16)


def attend_back(length, proj, d_heads, heads_out, lse, heads, block=512):
    seq, width = proj.shape[0], proj.shape[1] // 3
    pairs, head_dim = heads // 2, width // heads
    two = 2 * head_dim

    def part(n):
        return pl.BlockSpec((seq, two), lambda p: (0, n * pairs + p))

    one = pl.BlockSpec((seq, two), lambda p: (0, p))
    return pl.pallas_call(
        functools.partial(attend_back_kernel, head_dim, block),
        grid=(pairs,),
        out_shape=[jax.ShapeDtypeStruct((seq, width), jnp.bfloat16)] * 3,
        in_specs=[pl.BlockSpec(memory_space=pltpu.SMEM), part(0), part(1), part(2), one, one, one],
        out_specs=[one] * 3,
        scratch_shapes=[
            pltpu.VMEM((2, seq, 2 * two), jnp.bfloat16),
            pltpu.VMEM((2, seq, 2 * two), jnp.bfloat16),
            pltpu.VMEM((2, seq, two), jnp.bfloat16),
            pltpu.VMEM((2, seq, two), jnp.bfloat16),
            pltpu.VMEM((2, seq, two), jnp.float32),
            pltpu.VMEM((2, seq, two), jnp.float32),
            pltpu.VMEM((two, seq), jnp.bfloat16),
        ],
        compiler_params=pltpu.CompilerParams(vmem_limit_bytes=56 << 20),
        name="attend_bwd",
    )(length, proj, proj, proj, d_heads, heads_out, lse)

def erf_of(x):
    x = jnp.clip(x, -3.7439211627767994, 3.7439211627767994)
    s = x * x
    top = 0.00022905065861350646
    for c in (0.0034082910107109506, 0.050955695062380861, 0.18520832239976145, 1.128379143519084):
        top = top * s + c
    low = -1.1791602954361697e-7
    for c in (
        0.000023547966471313185,
        0.0010179625278914885,
        0.014070470171167667,
        0.11098505178285362,
        0.49746925110067538,
        1.0,
    ):
        low = low * s + c
    return x * top / low


def centre(h):
    shifted = h - jnp.mean(h, axis=1, keepdims=True)
    scale = lax.rsqrt(jnp.mean(shifted * shifted, axis=1, keepdims=True) + EPSILON)
    return shifted * scale, scale


def centre_back(dy, gain, hat, scale):
    d = dy * gain
    return scale * (
        d - jnp.mean(d, axis=1, keepdims=True) - hat * jnp.mean(d * hat, axis=1, keepdims=True)
    )


def middle_kernel(
    chunk, length_ref, drop_ref, x_ref, cot_ref, o_ref, w_out, w_up, w_down, vec, b_up,
    result_ref, dh1_ref, do_ref, act_ref, du_ref, x1_ref, df_ref, da_ref, dvec, db_up, slope,
):
    f32, bf16 = jnp.float32, jnp.bfloat16
    rows = x_ref.shape[0]
    hidden = w_up.shape[1]
    step = pl.program_id(0)
    row = step * rows + lax.broadcasted_iota(jnp.int32, (rows, 1), 0)
    live = jnp.where(row < length_ref[0], 1.0, 0.0)
    keep = (1 - drop_ref[0]).astype(f32)
    b_out, g1, s1, b_down, g2, s2 = [vec[n : n + 1, :] for n in range(2, 8)]
    across = (((1,), (1,)), ((), ()))

    @pl.when(step == 0)
    def _():
        dvec[...] = jnp.zeros_like(dvec)
        db_up[...] = jnp.zeros_like(db_up)

    x = x_ref[...].astype(f32)
    h1 = x + (jnp.dot(o_ref[...], w_out[...], preferred_element_type=f32) + b_out)
    hat1, scale1 = centre(h1)
    x1 = hat1 * g1 + s1
    x1_low = x1.astype(bf16)
    x1_ref[...] = x1_low
    ff = b_down
    for n in range(0, hidden, chunk):
        at = slice(n, n + chunk)
        u = jnp.dot(x1_low, w_up[:, at], preferred_element_type=f32) + b_up[:, at]
        upper = 0.5 + 0.5 * erf_of(u * 0.7071067811865476)
        slope[:, at] = upper + u * (0.3989422804014327 * jnp.exp(-0.5 * (u * u)))
        act = (u * upper).astype(bf16)
        act_ref[:, at] = act
        ff = ff + jnp.dot(act, w_down[at, :], preferred_element_type=f32)
    h2 = x1 + ff
    hat2, scale2 = centre(h2)
    result_ref[...] = (live * (keep * (hat2 * g2 + s2) + (1 - keep) * x)).astype(bf16)
    dy = (keep * live) * cot_ref[...].astype(f32)
    dh2 = centre_back(dy, g2, hat2, scale2)
    df = dh2.astype(bf16)
    df_ref[...] = df
    dvec[5:6, :] += jnp.sum(df.astype(f32), axis=0, keepdims=True)
    dvec[6:7, :] += jnp.sum(dy * hat2, axis=0, keepdims=True)
    dvec[7:8, :] += jnp.sum(dy, axis=0, keepdims=True)
    dx1 = dh2
    for n in range(0, hidden, chunk):
        at = slice(n, n + chunk)
        da_ff = lax.dot_general(df, w_down[at, :], across, preferred_element_type=f32)
        du = (da_ff * slope[:, at]).astype(bf16)
        du_ref[:, at] = du
        db_up[:, at] += jnp.sum(du.astype(f32), axis=0, keepdims=True)
        dx1 = dx1 + lax.dot_general(du, w_up[:, at], across, preferred_element_type=f32)
    dvec[3:4, :] += jnp.sum(dx1 * hat1, axis=0, keepdims=True)
    dvec[4:5, :] += jnp.sum(dx1, axis=0, keepdims=True)
    dh1 = centre_back(dx1, g1, hat1, scale1)
    dh1_ref[...] = dh1
    da = dh1.astype(bf16)
    da_ref[...] = da
    dvec[2:3, :] += jnp.sum(da.astype(f32), axis=0, keepdims=True)
    do_ref[...] = lax.dot_general(da, w_out[...], across, preferred_element_type=f32).astype(bf16)


def middle(length, drop, tokens, cotangent, heads_out, w_out, w_up, w_down, vec, b_up, block=256, chunk=768):
    seq, width = tokens.shape
    hidden = w_up.shape[1]
    f32, bf16 = jnp.float32, jnp.bfloat16
    smem = pl.BlockSpec(memory_space=pltpu.SMEM)
    thin = pl.BlockSpec((block, width), lambda i: (i, 0))
    wide = pl.BlockSpec((block, hidden), lambda i: (i, 0))

    def whole(shape):
        return pl.BlockSpec(shape, lambda i: (0, 0), pipeline_mode=pl.Buffered(1))

    def like(cols, dtype):
        return jax.ShapeDtypeStruct((seq, cols), dtype)

    return pl.pallas_call(
        functools.partial(middle_kernel, chunk),
        grid=(seq // block,),
        out_shape=[
            like(width, bf16),
            like(width, f32),
            like(width, bf16),
            like(hidden, bf16),
            like(hidden, bf16),
            like(width, bf16),
            like(width, bf16),
            like(width, bf16),
            jax.ShapeDtypeStruct((8, width), f32),
            jax.ShapeDtypeStruct((1, hidden), f32),
        ],
        in_specs=[smem, smem, thin, thin, thin]
        + [whole(w.shape) for w in (w_out, w_up, w_down, vec, b_up)],
        out_specs=[thin, thin, thin, wide, wide, thin, thin, thin]
        + [pl.BlockSpec(s, lambda i: (0, 0)) for s in ((8, width), (1, hidden))],
        scratch_shapes=[
            pltpu.VMEM((block, hidden), f32),
        ],
        compiler_params=pltpu.CompilerParams(vmem_limit_bytes=60 << 20),
        name="middle",
    )(length, drop, tokens, cotangent, heads_out, w_out, w_up, w_down, vec, b_up)

def tail_kernel(
    length_ref, drop_ref, dq_ref, dk_ref, dv_ref, dh1_ref, cot_ref, w_ref, out_ref, sums
):
    f32 = jnp.float32
    rows, width = dh1_ref.shape
    step = pl.program_id(0)
    row = step * rows + lax.broadcasted_iota(jnp.int32, (rows, 1), 0)
    live = jnp.where(row < length_ref[0], 1.0, 0.0)
    keep = (1 - drop_ref[0]).astype(f32)
    across = (((1,), (1,)), ((), ()))

    @pl.when(step == 0)
    def _():
        sums[...] = jnp.zeros_like(sums)

    total = dh1_ref[...]
    for n, part in enumerate((dq_ref, dk_ref, dv_ref)):
        total = total + lax.dot_general(
            part[...], w_ref[:, n * width : (n + 1) * width], across, preferred_element_type=f32
        )
    out_ref[...] = keep * total + ((1 - keep) * live) * cot_ref[...].astype(f32)
    sums[0:1, :] += jnp.sum(dq_ref[...].astype(f32), axis=0, keepdims=True)
    sums[1:2, :] += jnp.sum(dv_ref[...].astype(f32), axis=0, keepdims=True)


def tail(length, drop, dq, dk, dv, dh1, cotangent, w_qkv, block=256):
    seq, width = dq.shape
    smem = pl.BlockSpec(memory_space=pltpu.SMEM)
    thin = pl.BlockSpec((block, width), lambda i: (i, 0))
    weight = pl.BlockSpec(w_qkv.shape, lambda i: (0, 0), pipeline_mode=pl.Buffered(1))
    return pl.pallas_call(
        tail_kernel,
        grid=(seq // block,),
        out_shape=[
            jax.ShapeDtypeStruct((seq, width), jnp.float32),
            jax.ShapeDtypeStruct((8, width), jnp.float32),
        ],
        in_specs=[smem, smem, thin, thin, thin, thin, thin, weight],
        out_specs=[thin, pl.BlockSpec((8, width), lambda i: (0, 0))],
        compiler_params=pltpu.CompilerParams(vmem_limit_bytes=40 << 20),
        name="grad_tokens",
    )(length, drop, dq, dk, dv, dh1, cotangent, w_qkv)

def pack(attn_vectors, ffn_vectors, up_bias):
    rows = jnp.concatenate([attn_vectors.T, ffn_vectors.T], axis=0).reshape(-1)
    return jnp.concatenate([rows, up_bias])


def unpack(shares, rows):
    devices = shares.shape[0]
    vec = shares[:, : 8 * rows].reshape(devices, 8, rows).transpose(1, 0, 2)
    hidden = shares[:, 8 * rows : 12 * rows].reshape(1, -1)
    return vec.reshape(8, -1).astype(jnp.float32), hidden.astype(jnp.float32)


def repack(d_vec, d_hidden, devices):
    rows = d_vec.shape[1] // devices
    vec = d_vec.reshape(8, devices, rows).transpose(1, 0, 2).reshape(devices, -1)
    return jnp.concatenate([vec, d_hidden.reshape(devices, -1)], axis=1)


def fetch_plain(w_qkv, w_out, w_up, w_down, small):
    weights = tuple(
        lax.all_gather(w, "dp", axis=0, tiled=True) for w in (w_qkv, w_out, w_up, w_down)
    )
    return (*weights, lax.all_gather(small, "dp", axis=0))


def spread_plain(grads, small):
    f32 = jnp.float32
    sums = [lax.psum_scatter(g.astype(f32), "dp", scatter_dimension=0, tiled=True) for g in grads]
    return sums, lax.psum_scatter(small, "dp", scatter_dimension=0)


def fetch_kernel(w_qkv, w_out, w_up, w_down, small):
    share = small.shape[0]
    small = jnp.pad(small, (0, 16 * LANES - share)).reshape(16, LANES)
    full = gather([w_qkv, w_out, w_up, w_down, small])
    weights = tuple(f.reshape(-1, f.shape[-1]) for f in full[:4])
    return (*weights, full[4].reshape(-1, 16 * LANES)[:, :share])


def spread_kernel(grads, small):
    devices, share = small.shape
    small = jnp.pad(small, ((0, 0), (0, 16 * LANES - share))).astype(jnp.bfloat16)
    sums = scatter([as_slabs(g) for g in grads] + [small.reshape(GRID + (16, LANES))])
    back = [from_slab(s, g.shape[0] // devices, g.shape[1]) for s, g in zip(sums, grads)]
    return back, sums[-1].reshape(-1)[:share]


def transposed(left, right):
    return jnp.einsum("ta,tb->ab", left, right, preferred_element_type=jnp.float32).astype(
        jnp.bfloat16
    )


def local(
    fetch,
    spread,
    tokens,
    lengths,
    drops,
    cotangent,
    w_qkv,
    w_out,
    w_up,
    w_down,
    attn_vectors,
    ffn_vectors,
    up_bias,
):
    f32, bf16 = jnp.float32, jnp.bfloat16
    rows = w_qkv.shape[0]
    width = tokens.shape[1]
    qkv_full, out_full, up_full, down_full, shares = fetch(
        w_qkv, w_out, w_up, w_down, pack(attn_vectors, ffn_vectors, up_bias)
    )
    vec, b_up = unpack(shares, rows)
    qkv_bias = jnp.concatenate([vec[0], jnp.zeros((width,), f32), vec[1]])
    proj = (jnp.dot(tokens, qkv_full, preferred_element_type=f32) + qkv_bias).astype(bf16)
    heads_out, log_sums = attend(lengths, proj, H)
    result, dh1, d_heads, act, d_pre, x1, d_ff, d_attn, d_vec, d_up_bias = middle(
        lengths, drops, tokens, cotangent, heads_out, out_full, up_full, down_full, vec, b_up
    )
    dq, dk, dv = attend_back(lengths, proj, d_heads, heads_out, log_sums, H)
    grad_tokens, proj_sums = tail(lengths, drops, dq, dk, dv, dh1, cotangent, qkv_full)
    grads = [transposed(tokens, d) for d in (dq, dk, dv)]
    grads += [transposed(heads_out, d_attn), transposed(x1, d_pre), transposed(act, d_ff)]
    small = repack(d_vec + proj_sums, d_up_bias, lax.axis_size("dp"))
    sums, small = spread(grads, small)
    d_vec, d_up_bias = small[: 8 * rows].reshape(8, rows), small[8 * rows :]
    return (
        result,
        grad_tokens,
        jnp.concatenate(sums[:3], axis=1),
        sums[3],
        sums[4],
        sums[5],
        d_vec[:5].T,
        d_vec[5:].T,
        d_up_bias,
    )


def solution(mesh):
    kernels = mesh.shape["dp"] == 32
    layer = functools.partial(
        local, fetch_kernel if kernels else fetch_plain, spread_kernel if kernels else spread_plain
    )
    rows, line = P("dp", None), P("dp")
    return jax.shard_map(
        layer,
        mesh=mesh,
        in_specs=(rows, line, line, rows, rows, rows, rows, rows, rows, rows, line),
        out_specs=(rows, rows, rows, rows, rows, rows, rows, rows, line),
        check_vma=False,
    )
```
